32 devices in a mesh: groups: 2 (over x), blk: 16 (over z, y, core).
Axes of the slice: x: 2, y: 2, z: 4, core: 2. Of those that a mesh axis runs over, the one named last changes fastest.
Arguments:
- pair_elements: float32 [12288, 1024], P(('groups', 'blk')), parts along dimension 0, may hold values from -0.8 to 0.8
- gmap: int32 [12288], P(('groups', 'blk')), parts along dimension 0, may hold values from 0 to 6143, as said below
- w_screened: float32 [12288, 6144], P('groups', 'blk'), parts along dimension 0, as said below
- coulomb: float32 [12288], P(('groups', 'blk')), parts along dimension 0, may hold values from 0.001 to 0.02
Outputs:
- screened: float32 [12288, 1024], P(('groups', 'blk')), parts along dimension 0
- pair_sigma: float32 [2048], P(('groups', 'blk')), parts along dimension 0
The draws below stay inside these ranges and needn't reach their ends.
There are 2 independent parts, one for each index of `groups`. The reference program is written for one: setup_inputs(seed, part) draws one part's arguments, and reference() takes and returns one part's arrays. A program takes and returns all parts, laid end to end along the dimension named above; each array names one. Nothing has to cross between parts.
Inputs may be any that keep to these rules, and one draw needn't show every extreme that they name: `gmap`: each aligned block of 384 entries is a permutation of that block's own indices. `w_screened`: symmetric.
All inputs are finite; a program needn't handle non-finite values.
Results may differ from the reference program's by a relative error of at most 0.00013.
Values sent between devices are 32-bit elements; how exact they have to be, the bound alone decides.
A program may use at most 256 MiB of HBM per device.

```python
import math
import jax
import jax.numpy as jnp
from jax import lax

G_DEV = 384
NG = 6144
NB = 64
OCC = 4
P_SIZE = 1024


def draw_gmap(key, part):
    blocks = NG // G_DEV
    scores = jax.random.randint(key, (blocks, G_DEV), 0, 1 << 30)
    scores = scores * G_DEV + jnp.arange(G_DEV, dtype=jnp.int32)[None, :]
    order = jnp.argsort(scores, axis=1, stable=True).astype(jnp.int32)
    offsets = (jnp.arange(blocks, dtype=jnp.int32) * G_DEV)[:, None]
    return (order + offsets).reshape(NG).astype(jnp.int32)


def draw_w_screened(key, part):
    base = jax.random.normal(key, (NG, NG), jnp.float32)
    return ((base + base.T) * (0.5 / NG) ** 0.5).astype(jnp.float32)


def raised(entries, own_key, source, target, shards_of, factor):
    def block_of(dim):
        return (jnp.arange(entries.shape[dim]) // (entries.shape[dim] // shards_of)).reshape((-1,) + (1,) * (entries.ndim - 1 - dim))

    first = jax.random.permutation(own_key, shards_of)[block_of(target)]
    far = (block_of(target) + shards_of // 2) % shards_of
    return jnp.where((block_of(source) == first) | (block_of(source) == far), factor * entries, entries)


def steps_of(key, dims, shards, smallest, top_value):
    level, own = 1.0, jax.random.fold_in(key, 6)
    for axis_at, shards_of in shards:
        steps = jnp.exp(jax.random.uniform(jax.random.fold_in(own, axis_at), (shards_of,), jnp.float32, smallest / len(shards), top_value / len(shards)))
        level = level * jnp.repeat(steps, dims[axis_at] // shards_of).reshape([-1 if axis == axis_at else 1 for axis in range(len(dims))])
    return level


def noise_with(own_key, dims, deviation, reach, cuts, heavy, kind=jnp.bfloat16):
    result = deviation * jax.random.normal(own_key, dims, jnp.float32)
    if cuts:
        result = result * steps_of(own_key, dims, cuts, -0.22, 0.18)
    return jnp.clip(raised(result, jax.random.fold_in(own_key, 3), *heavy), -reach, reach).astype(kind)


def setup_inputs(seed: int = 0, part: int = 0) -> dict:
    key_list = jax.random.split(jax.random.key(seed), 5)
    part_keys = jax.random.split(jax.random.fold_in(key_list[4], part), 5)
    return {
        "pair_elements": noise_with(part_keys[0], (NG, P_SIZE), 0.1, 0.8, ((0, 16),), (0, 1, 16, 2.0), jnp.float32),
        "gmap": draw_gmap(jax.random.fold_in(jax.random.fold_in(key_list[4], part), 71), part),
        "w_screened": draw_w_screened(jax.random.fold_in(jax.random.fold_in(key_list[4], part), 71), part),
        "coulomb": jnp.clip(jnp.exp(math.log(0.02) - 2.9957322 * jax.random.uniform(part_keys[3], (NG,), jnp.float32) ** steps_of(part_keys[3], (NG,), ((0, 16),), -0.2, 0.2)), 0.001, 0.02),
    }


def reference(pair_elements, gmap, w_screened, coulomb):
    elements = jnp.take(pair_elements, gmap.astype(jnp.int32), axis=0)
    screened = lax.dot_general(w_screened, elements, (((0,), (0,)), ((), ())), precision=lax.Precision.HIGHEST, preferred_element_type=jnp.float32)
    band = jnp.arange(P_SIZE, dtype=jnp.int32) % NB
    coef = jnp.where(band < OCC, -0.5, 0.5).astype(jnp.float32)
    pair_sigma = coef * jnp.sum(screened * elements, axis=0) - 0.5 * jnp.sum(coulomb[:, None] * elements * elements, axis=0)
    return screened, pair_sigma
```

```python
import functools

import jax
import jax.numpy as jnp
from jax import lax
from jax.experimental import pallas as pl
from jax.experimental.pallas import tpu as pltpu
from jax.sharding import PartitionSpec as P

NB = 64
OCC = 4
ROWS_Y = 2
CORES = 2
CHUNKS = 6
VMEM_ROOM = 58 * 2**20


def dot3(w, e):
    wt = w.T
    wh = wt.astype(jnp.bfloat16)
    wl = (wt - wh.astype(jnp.float32)).astype(jnp.bfloat16)
    eh = e.astype(jnp.bfloat16)
    el = (e - eh.astype(jnp.float32)).astype(jnp.bfloat16)
    dot = functools.partial(jnp.dot, preferred_element_type=jnp.float32)
    return dot(wl, eh) + dot(wh, el) + dot(wh, eh)


def kernel(depth, e_hbm, w_hbm, c_ref, out_ref, sig_ref, ez, ey, wbuf, parts, load_sem, s_y, s_up, s_dn, s_d2d, r_sem, p_send, p_recv):
    n = depth * ROWS_Y * CORES
    me = lax.axis_index("blk")
    z = me // (ROWS_Y * CORES)
    y = (me // CORES) % ROWS_Y
    c = me % CORES
    oy, oc = 1 - y, 1 - c
    head = ey.shape[1]
    body_rows = ez.shape[1]
    cols = ez.shape[2]

    def blk(zz, yy, cc):
        return (zz * ROWS_Y + yy) * CORES + cc

    own_y = pltpu.make_async_copy(e_hbm.at[pl.ds(0, head)], ey.at[me], load_sem.at[0])
    own_z = pltpu.make_async_copy(e_hbm.at[pl.ds(head, body_rows)], ez.at[me], load_sem.at[1])
    w_in = pltpu.make_async_copy(w_hbm, wbuf, load_sem.at[2])
    own_y.start()
    own_z.start()
    w_in.start()

    barrier = pltpu.get_barrier_semaphore()

    @pl.loop(1, n)
    def _(j):
        pl.semaphore_signal(barrier, inc=1, device_id={"blk": (me + j) % n}, device_id_type=pl.DeviceIdType.MESH)

    pl.semaphore_wait(barrier, n - 1)
    own_y.wait()
    own_z.wait()

    def piece(b, k):
        return ez.at[b, pl.ds(pl.multiple_of((k - 1) * head, head), head)]

    def rdma(ref, send, b, k, target):
        return pltpu.make_async_remote_copy(
            src_ref=ref, dst_ref=ref, send_sem=send, recv_sem=r_sem.at[b, k],
            device_id={"blk": target}, device_id_type=pl.DeviceIdType.MESH)

    def copy(kind, b, k, ref):
        zz, yy = b // (ROWS_Y * CORES), (b // CORES) % ROWS_Y
        if kind == "y":
            return rdma(ref, s_y.at[zz, k], b, k, blk(z, oy, c))
        if kind == "up":
            return rdma(ref, s_up.at[b // CORES, k], b, k, blk((z + 1) % depth, y, c))
        if kind == "dn":
            return rdma(ref, s_dn.at[b // CORES, k], b, k, blk((z + depth - 1) % depth, y, c))
        return rdma(ref, s_d2d.at[b // CORES, k], b, k, blk(z, y, oc))

    def landed(b, k, ref):
        rdma(ref, s_y.at[0, 0], b, k, blk(z, y, oc)).wait_recv()

    copy("y", me, 0, ey.at[me]).start()

    @pl.loop(1, CHUNKS)
    def _(k):
        @pl.when(z > 0)
        def _():
            copy("dn", me, k, piece(me, k)).start()

        @pl.when(z < depth - 1)
        def _():
            copy("up", me, k, piece(me, k)).start()

        copy("y", me, k, piece(me, k)).start()
        copy("d2d", me, k, piece(me, k)).start()

    copy("d2d", me, 0, ey.at[me]).start()
    out_ref[...] = jnp.zeros_like(out_ref)
    w_in.wait()

    other = blk(z, oy, c)
    landed(other, 0, ey.at[other])
    copy("d2d", other, 0, ey.at[other]).start()

    @pl.loop(0, depth + 1)
    def _(d):
        @pl.when(jnp.logical_and(d >= 1, d < depth))
        def _():
            @pl.loop(1, CHUNKS)
            def _(k):
                @pl.when(z + d < depth)
                def _():
                    b = blk((z + d) % depth, y, c)
                    landed(b, k, piece(b, k))

                    @pl.when(z > 0)
                    def _():
                        copy("dn", b, k, piece(b, k)).start()

                    copy("y", b, k, piece(b, k)).start()
                    copy("d2d", b, k, piece(b, k)).start()

                @pl.when(z - d >= 0)
                def _():
                    b = blk((z - d + depth) % depth, y, c)
                    landed(b, k, piece(b, k))

                    @pl.when(z < depth - 1)
                    def _():
                        copy("up", b, k, piece(b, k)).start()

                    copy("y", b, k, piece(b, k)).start()
                    copy("d2d", b, k, piece(b, k)).start()

        @pl.when(jnp.logical_and(z + d == depth - 1, z > 0))
        def _():
            copy("dn", me, 0, ey.at[me]).start()
            copy("dn", other, 0, ey.at[other]).start()

        @pl.when(jnp.logical_and(z - d == 0, z < depth - 1))
        def _():
            copy("up", me, 0, ey.at[me]).start()
            copy("up", other, 0, ey.at[other]).start()

        @pl.loop(0, 8)
        def _(i):
            cross = i // 4
            sign = (i // 2) % 2
            far = i % 2
            dist = d - cross
            zz = z + (2 * sign - 1) * dist
            ok = jnp.logical_and(dist >= 0, jnp.logical_or(sign == 0, dist > 0))
            ok = jnp.logical_and(ok, jnp.logical_and(zz >= 0, zz < depth))

            @pl.when(ok)
            def _():
                at = (zz + 2 * depth) % depth
                yy = (y + cross) % ROWS_Y
                cc = (c + far) % CORES
                b = blk(at, yy, cc)

                @pl.when(far == 1)
                def _():
                    @pl.loop(1, CHUNKS)
                    def _(k):
                        landed(b, k, piece(b, k))

                @pl.when(jnp.logical_and(far == 0, cross == 1))
                def _():
                    @pl.loop(1, CHUNKS)
                    def _(k):
                        landed(b, k, piece(b, k))
                        copy("d2d", b, k, piece(b, k)).start()

                out_ref[...] += dot3(wbuf[b, head:, :], ez[b])

    def first_pieces(zz):
        rows = ROWS_Y * CORES * head
        w = wbuf[pl.ds(zz * ROWS_Y * CORES, ROWS_Y * CORES), :head, :].reshape(rows, wbuf.shape[2])
        e = ey[pl.ds(zz * ROWS_Y * CORES, ROWS_Y * CORES)].reshape(rows, cols)
        out_ref[...] += dot3(w, e)

    @pl.loop(0, depth)
    def _(d):
        @pl.loop(0, 2)
        def _(sign):
            zz = z + (2 * sign - 1) * d
            ok = jnp.logical_and(jnp.logical_or(sign == 0, d > 0), jnp.logical_and(zz >= 0, zz < depth))

            @pl.when(ok)
            def _():
                at = (zz + depth) % depth

                @pl.when(d > 0)
                def _():
                    @pl.loop(0, ROWS_Y)
                    def _(j):
                        b = blk(at, (y + j) % ROWS_Y, c)
                        landed(b, 0, ey.at[b])

                        @pl.when(jnp.logical_and(sign == 1, z > 0))
                        def _():
                            copy("dn", b, 0, ey.at[b]).start()

                        @pl.when(jnp.logical_and(sign == 0, z < depth - 1))
                        def _():
                            copy("up", b, 0, ey.at[b]).start()

                        copy("d2d", b, 0, ey.at[b]).start()

                @pl.loop(0, ROWS_Y)
                def _(yy):
                    b = blk(at, yy, oc)
                    landed(b, 0, ey.at[b])

                first_pieces(at)

    own_head, own_body = ey[me], ez[me]
    coul = jnp.broadcast_to(c_ref[...], (128, c_ref.shape[1])).T[:, :1]
    band = lax.broadcasted_iota(jnp.int32, (1, cols), 1) % NB
    coef = jnp.where(band < OCC, -0.5, 0.5).astype(jnp.float32)
    screened_sum = jnp.sum(out_ref[:head, :] * own_head, axis=0, keepdims=True) + jnp.sum(
        out_ref[head:, :] * own_body, axis=0, keepdims=True)
    bare_sum = jnp.sum(coul[:head] * own_head * own_head, axis=0, keepdims=True) + jnp.sum(
        coul[head:] * own_body * own_body, axis=0, keepdims=True)
    parts[me] = coef * screened_sum - 0.5 * bare_sum

    def part_copy(source, target, j):
        return pltpu.make_async_remote_copy(
            src_ref=parts.at[source], dst_ref=parts.at[source], send_sem=p_send.at[j], recv_sem=p_recv.at[source],
            device_id={"blk": target}, device_id_type=pl.DeviceIdType.MESH)

    @pl.loop(1, n)
    def _(j):
        part_copy(me, (me + j) % n, j).start()

    @pl.loop(1, n)
    def _(j):
        part_copy((me + j) % n, (me + j) % n, j).wait_recv()

    sig_ref[...] = jnp.sum(parts[...], axis=0)

    @pl.loop(1, n)
    def _(j):
        part_copy(me, (me + j) % n, j).wait_send()

    @pl.loop(0, n // CORES)
    def _(h):
        zz, yy = h // ROWS_Y, h % ROWS_Y
        b = h * CORES + c

        def sent(kind, k, ref):
            copy(kind, b, k, ref).wait_send()

        @pl.loop(1, CHUNKS)
        def _(k):
            sent("d2d", k, piece(b, k))

            @pl.when(yy == y)
            def _():
                sent("y", k, piece(b, k))

                @pl.when(jnp.logical_and(zz >= z, z > 0))
                def _():
                    sent("dn", k, piece(b, k))

                @pl.when(jnp.logical_and(zz <= z, z < depth - 1))
                def _():
                    sent("up", k, piece(b, k))

        sent("d2d", 0, ey.at[b])

        @pl.when(b == me)
        def _():
            sent("y", 0, ey.at[b])

        @pl.when(jnp.logical_and(zz >= z, z > 0))
        def _():
            sent("dn", 0, ey.at[b])

        @pl.when(jnp.logical_and(zz <= z, z < depth - 1))
        def _():
            sent("up", 0, ey.at[b])


def fused(n, elements, w_screened, coulomb):
    rows, cols = elements.shape
    head = rows // CHUNKS
    depth = n // (ROWS_Y * CORES)
    f32 = jnp.float32
    half = n // CORES
    dma = pltpu.SemaphoreType.DMA
    screened, sig = pl.pallas_call(
        functools.partial(kernel, depth),
        out_shape=(jax.ShapeDtypeStruct((rows, cols), f32), jax.ShapeDtypeStruct((1, cols), f32)),
        in_specs=[pl.BlockSpec(memory_space=pl.ANY), pl.BlockSpec(memory_space=pl.ANY), pl.BlockSpec(memory_space=pltpu.VMEM)],
        out_specs=(pl.BlockSpec(memory_space=pltpu.VMEM), pl.BlockSpec(memory_space=pltpu.VMEM)),
        scratch_shapes=[
            pltpu.VMEM((n, rows - head, cols), f32),
            pltpu.VMEM((n, head, cols), f32),
            pltpu.VMEM((n, rows, rows), f32),
            pltpu.VMEM((n, 1, cols), f32),
            dma((3,)),
            dma((depth, CHUNKS)),
            dma((half, CHUNKS)),
            dma((half, CHUNKS)),
            dma((half, CHUNKS)),
            dma((n, CHUNKS)),
            dma((n,)),
            dma((n,)),
        ],
        compiler_params=pltpu.CompilerParams(collective_id=0, has_side_effects=True, vmem_limit_bytes=60 * 2**20),
        name="gather_matmul",
    )(elements, w_screened.reshape(n, rows, rows), coulomb.reshape(1, rows))
    me = lax.axis_index("blk")
    pair_sigma = lax.dynamic_slice(sig.reshape(cols), (me * (cols // n),), (cols // n,))
    return screened, pair_sigma


def plain(elements, w_screened, coulomb):
    screened = lax.dot_general(
        w_screened,
        lax.all_gather(elements, "blk", axis=0, tiled=True),
        (((0,), (0,)), ((), ())),
        precision=lax.Precision.HIGHEST,
        preferred_element_type=jnp.float32,
    )
    band = jnp.arange(elements.shape[1], dtype=jnp.int32) % NB
    coef = jnp.where(band < OCC, -0.5, 0.5).astype(jnp.float32)
    partial_terms = coef * jnp.sum(screened * elements, axis=0) - 0.5 * jnp.sum(
        coulomb[:, None] * elements * elements, axis=0
    )
    pair_sigma = lax.psum_scatter(partial_terms, "blk", scatter_dimension=0, tiled=True)
    return screened, pair_sigma


def solution(mesh):
    n = mesh.shape["blk"]

    def local(pair_elements, gmap, w_screened, coulomb):
        rows, cols = pair_elements.shape
        elements = jnp.take(pair_elements, gmap % rows, axis=0, mode="clip")
        held = 4 * n * rows * (cols + rows) + 4 * 3 * rows * cols
        fits = held < VMEM_ROOM and n % (ROWS_Y * CORES) == 0 and rows % (8 * CHUNKS) == 0
        if fits:
            return fused(n, elements, w_screened, coulomb)
        return plain(elements, w_screened, coulomb)

    in_specs = (
        P(("groups", "blk"), None),
        P(("groups", "blk")),
        P("groups", "blk"),
        P(("groups", "blk")),
    )
    out_specs = (P(("groups", "blk"), None), P(("groups", "blk")))
    return jax.shard_map(local, mesh=mesh, in_specs=in_specs, out_specs=out_specs, check_vma=False)
```

```python
import functools

import jax
import jax.numpy as jnp
from jax import lax
from jax.experimental import pallas as pl
from jax.experimental.pallas import tpu as pltpu
from jax.sharding import PartitionSpec as P

NB = 64
OCC = 4
ROWS_Y = 2
CORES = 2
CHUNKS = 4
VMEM_ROOM = 58 * 2**20


def dot3(w, e):
    wt = w.T
    wh = wt.astype(jnp.bfloat16)
    wl = (wt - wh.astype(jnp.float32)).astype(jnp.bfloat16)
    eh = e.astype(jnp.bfloat16)
    el = (e - eh.astype(jnp.float32)).astype(jnp.bfloat16)
    dot = functools.partial(jnp.dot, preferred_element_type=jnp.float32)
    return dot(wl, eh) + dot(wh, el) + dot(wh, eh)


def kernel(depth, e_hbm, w_hbm, c_ref, out_ref, sig_ref, ez, ey, wbuf, parts, load_sem, s_y, s_up, s_dn, s_d2d, r_sem, p_send, p_recv):
    n = depth * ROWS_Y * CORES
    me = lax.axis_index("blk")
    z = me // (ROWS_Y * CORES)
    y = (me // CORES) % ROWS_Y
    c = me % CORES
    oy, oc = 1 - y, 1 - c
    head = ey.shape[1]
    body_rows = ez.shape[1]
    step = body_rows // (CHUNKS - 1)
    cols = ez.shape[2]

    def blk(zz, yy, cc):
        return (zz * ROWS_Y + yy) * CORES + cc

    own_y = pltpu.make_async_copy(e_hbm.at[pl.ds(0, head)], ey.at[me], load_sem.at[0])
    own_z = pltpu.make_async_copy(e_hbm.at[pl.ds(head, body_rows)], ez.at[me], load_sem.at[1])
    w_in = pltpu.make_async_copy(w_hbm, wbuf, load_sem.at[2])
    own_y.start()
    own_z.start()
    w_in.start()

    barrier = pltpu.get_barrier_semaphore()

    @pl.loop(1, n)
    def _(j):
        pl.semaphore_signal(barrier, inc=1, device_id={"blk": (me + j) % n}, device_id_type=pl.DeviceIdType.MESH)

    pl.semaphore_wait(barrier, n - 1)
    own_y.wait()
    own_z.wait()

    def piece(b, k):
        return ez.at[b, pl.ds(pl.multiple_of((k - 1) * step, step), step)]

    def rdma(ref, send, b, k, target):
        return pltpu.make_async_remote_copy(
            src_ref=ref, dst_ref=ref, send_sem=send, recv_sem=r_sem.at[b, k],
            device_id={"blk": target}, device_id_type=pl.DeviceIdType.MESH)

    def copy(kind, b, k, ref):
        zz, yy = b // (ROWS_Y * CORES), (b // CORES) % ROWS_Y
        if kind == "y":
            return rdma(ref, s_y.at[zz, k], b, k, blk(z, oy, c))
        if kind == "up":
            return rdma(ref, s_up.at[b // CORES, k], b, k, blk((z + 1) % depth, y, c))
        if kind == "dn":
            return rdma(ref, s_dn.at[b // CORES, k], b, k, blk((z + depth - 1) % depth, y, c))
        return rdma(ref, s_d2d.at[b // CORES, k], b, k, blk(z, y, oc))

    def landed(b, k, ref):
        rdma(ref, s_y.at[0, 0], b, k, blk(z, y, oc)).wait_recv()

    copy("y", me, 0, ey.at[me]).start()

    @pl.loop(1, CHUNKS)
    def _(k):
        @pl.when(z > 0)
        def _():
            copy("dn", me, k, piece(me, k)).start()

        @pl.when(z < depth - 1)
        def _():
            copy("up", me, k, piece(me, k)).start()

        copy("y", me, k, piece(me, k)).start()

    out_ref[...] = jnp.zeros_like(out_ref)
    w_in.wait()

    @pl.loop(1, CHUNKS)
    def _(k):
        copy("d2d", me, k, piece(me, k)).start()

    copy("d2d", me, 0, ey.at[me]).start()

    other = blk(z, oy, c)
    landed(other, 0, ey.at[other])
    copy("d2d", other, 0, ey.at[other]).start()

    def pass_first(at, kind):
        @pl.loop(0, ROWS_Y)
        def _(j):
            b = blk(at, (y + j) % ROWS_Y, c)
            landed(b, 0, ey.at[b])
            if kind is not None:
                copy(kind, b, 0, ey.at[b]).start()
            copy("d2d", b, 0, ey.at[b]).start()

    @pl.loop(0, depth + 1)
    def _(d):
        @pl.when(jnp.logical_and(d >= 1, d < depth))
        def _():
            @pl.loop(1, CHUNKS)
            def _(k):
                @pl.when(z + d < depth)
                def _():
                    b = blk((z + d) % depth, y, c)
                    landed(b, k, piece(b, k))

                    @pl.when(z > 0)
                    def _():
                        copy("dn", b, k, piece(b, k)).start()

                    copy("y", b, k, piece(b, k)).start()
                    copy("d2d", b, k, piece(b, k)).start()

                @pl.when(z - d >= 0)
                def _():
                    b = blk((z - d + depth) % depth, y, c)
                    landed(b, k, piece(b, k))

                    @pl.when(z < depth - 1)
                    def _():
                        copy("up", b, k, piece(b, k)).start()

                    copy("y", b, k, piece(b, k)).start()
                    copy("d2d", b, k, piece(b, k)).start()

        @pl.when(jnp.logical_and(z + d == depth - 1, z > 0))
        def _():
            copy("dn", me, 0, ey.at[me]).start()
            copy("dn", other, 0, ey.at[other]).start()

            @pl.loop(1, d + 1)
            def _(j):
                pass_first((z + j) % depth, "dn")

        @pl.when(jnp.logical_and(z - d == 0, z < depth - 1))
        def _():
            copy("up", me, 0, ey.at[me]).start()
            copy("up", other, 0, ey.at[other]).start()

            @pl.loop(1, d + 1)
            def _(j):
                pass_first((z - j + depth) % depth, "up")

        @pl.loop(0, 8)
        def _(i):
            cross = i // 4
            sign = (i // 2) % 2
            far = i % 2
            dist = d - cross
            zz = z + (2 * sign - 1) * dist
            ok = jnp.logical_and(dist >= 0, jnp.logical_or(sign == 0, dist > 0))
            ok = jnp.logical_and(ok, jnp.logical_and(zz >= 0, zz < depth))

            @pl.when(ok)
            def _():
                at = (zz + 2 * depth) % depth
                yy = (y + cross) % ROWS_Y
                cc = (c + far) % CORES
                b = blk(at, yy, cc)

                @pl.when(far == 1)
                def _():
                    @pl.loop(1, CHUNKS)
                    def _(k):
                        landed(b, k, piece(b, k))

                @pl.when(jnp.logical_and(far == 0, cross == 1))
                def _():
                    @pl.loop(1, CHUNKS)
                    def _(k):
                        landed(b, k, piece(b, k))
                        copy("d2d", b, k, piece(b, k)).start()

                out_ref[...] += dot3(wbuf[b, head:, :], ez[b])

    def first_pieces(zz):
        rows = ROWS_Y * CORES * head
        w = wbuf[pl.ds(zz * ROWS_Y * CORES, ROWS_Y * CORES), :head, :].reshape(rows, wbuf.shape[2])
        e = ey[pl.ds(zz * ROWS_Y * CORES, ROWS_Y * CORES)].reshape(rows, cols)
        out_ref[...] += dot3(w, e)

    @pl.loop(0, depth)
    def _(d):
        @pl.loop(0, 2)
        def _(sign):
            zz = z + (2 * sign - 1) * d
            ok = jnp.logical_and(jnp.logical_or(sign == 0, d > 0), jnp.logical_and(zz >= 0, zz < depth))

            @pl.when(ok)
            def _():
                at = (zz + depth) % depth

                end = jnp.logical_or(jnp.logical_and(sign == 1, z == 0), jnp.logical_and(sign == 0, z == depth - 1))

                @pl.when(jnp.logical_and(d > 0, end))
                def _():
                    pass_first(at, None)

                @pl.loop(0, ROWS_Y)
                def _(yy):
                    b = blk(at, yy, oc)
                    landed(b, 0, ey.at[b])

                first_pieces(at)

    own_head, own_body = ey[me], ez[me]
    coul = jnp.broadcast_to(c_ref[...], (128, c_ref.shape[1])).T[:, :1]
    band = lax.broadcasted_iota(jnp.int32, (1, cols), 1) % NB
    coef = jnp.where(band < OCC, -0.5, 0.5).astype(jnp.float32)
    screened_sum = jnp.sum(out_ref[:head, :] * own_head, axis=0, keepdims=True) + jnp.sum(
        out_ref[head:, :] * own_body, axis=0, keepdims=True)
    bare_sum = jnp.sum(coul[:head] * own_head * own_head, axis=0, keepdims=True) + jnp.sum(
        coul[head:] * own_body * own_body, axis=0, keepdims=True)
    parts[me] = coef * screened_sum - 0.5 * bare_sum

    def part_copy(source, target, j):
        return pltpu.make_async_remote_copy(
            src_ref=parts.at[source], dst_ref=parts.at[source], send_sem=p_send.at[j], recv_sem=p_recv.at[source],
            device_id={"blk": target}, device_id_type=pl.DeviceIdType.MESH)

    @pl.loop(1, n)
    def _(j):
        part_copy(me, (me + j) % n, j).start()

    @pl.loop(1, n)
    def _(j):
        part_copy((me + j) % n, (me + j) % n, j).wait_recv()

    sig_ref[...] = jnp.sum(parts[...], axis=0)

    @pl.loop(1, n)
    def _(j):
        part_copy(me, (me + j) % n, j).wait_send()

    @pl.loop(0, n // CORES)
    def _(h):
        zz, yy = h // ROWS_Y, h % ROWS_Y
        b = h * CORES + c

        def sent(kind, k, ref):
            copy(kind, b, k, ref).wait_send()

        @pl.loop(1, CHUNKS)
        def _(k):
            sent("d2d", k, piece(b, k))

            @pl.when(yy == y)
            def _():
                sent("y", k, piece(b, k))

                @pl.when(jnp.logical_and(zz >= z, z > 0))
                def _():
                    sent("dn", k, piece(b, k))

                @pl.when(jnp.logical_and(zz <= z, z < depth - 1))
                def _():
                    sent("up", k, piece(b, k))

        sent("d2d", 0, ey.at[b])

        @pl.when(b == me)
        def _():
            sent("y", 0, ey.at[b])

        @pl.when(jnp.logical_and(zz >= z, z > 0))
        def _():
            sent("dn", 0, ey.at[b])

        @pl.when(jnp.logical_and(zz <= z, z < depth - 1))
        def _():
            sent("up", 0, ey.at[b])


def head_rows(rows):
    return rows * 3 // 16


def fused(n, elements, w_screened, coulomb):
    rows, cols = elements.shape
    head = head_rows(rows)
    depth = n // (ROWS_Y * CORES)
    f32 = jnp.float32
    half = n // CORES
    dma = pltpu.SemaphoreType.DMA
    screened, sig = pl.pallas_call(
        functools.partial(kernel, depth),
        out_shape=(jax.ShapeDtypeStruct((rows, cols), f32), jax.ShapeDtypeStruct((1, cols), f32)),
        in_specs=[pl.BlockSpec(memory_space=pl.ANY), pl.BlockSpec(memory_space=pl.ANY), pl.BlockSpec(memory_space=pltpu.VMEM)],
        out_specs=(pl.BlockSpec(memory_space=pltpu.VMEM), pl.BlockSpec(memory_space=pltpu.VMEM)),
        scratch_shapes=[
            pltpu.VMEM((n, rows - head, cols), f32),
            pltpu.VMEM((n, head, cols), f32),
            pltpu.VMEM((n, rows, rows), f32),
            pltpu.VMEM((n, 1, cols), f32),
            dma((3,)),
            dma((depth, CHUNKS)),
            dma((half, CHUNKS)),
            dma((half, CHUNKS)),
            dma((half, CHUNKS)),
            dma((n, CHUNKS)),
            dma((n,)),
            dma((n,)),
        ],
        compiler_params=pltpu.CompilerParams(collective_id=0, has_side_effects=True, vmem_limit_bytes=60 * 2**20),
        name="gather_matmul",
    )(elements, w_screened.reshape(n, rows, rows), coulomb.reshape(1, rows))
    me = lax.axis_index("blk")
    pair_sigma = lax.dynamic_slice(sig.reshape(cols), (me * (cols // n),), (cols // n,))
    return screened, pair_sigma


def plain(elements, w_screened, coulomb):
    screened = lax.dot_general(
        w_screened,
        lax.all_gather(elements, "blk", axis=0, tiled=True),
        (((0,), (0,)), ((), ())),
        precision=lax.Precision.HIGHEST,
        preferred_element_type=jnp.float32,
    )
    band = jnp.arange(elements.shape[1], dtype=jnp.int32) % NB
    coef = jnp.where(band < OCC, -0.5, 0.5).astype(jnp.float32)
    partial_terms = coef * jnp.sum(screened * elements, axis=0) - 0.5 * jnp.sum(
        coulomb[:, None] * elements * elements, axis=0
    )
    pair_sigma = lax.psum_scatter(partial_terms, "blk", scatter_dimension=0, tiled=True)
    return screened, pair_sigma


def solution(mesh):
    n = mesh.shape["blk"]

    def local(pair_elements, gmap, w_screened, coulomb):
        rows, cols = pair_elements.shape
        elements = jnp.take(pair_elements, gmap % rows, axis=0, mode="clip")
        held = 4 * n * rows * (cols + rows) + 4 * 3 * rows * cols
        fits = held < VMEM_ROOM and n % (ROWS_Y * CORES) == 0 and rows % 128 == 0 and (rows - head_rows(rows)) % (8 * (CHUNKS - 1)) == 0
        if fits:
            return fused(n, elements, w_screened, coulomb)
        return plain(elements, w_screened, coulomb)

    in_specs = (
        P(("groups", "blk"), None),
        P(("groups", "blk")),
        P("groups", "blk"),
        P(("groups", "blk")),
    )
    out_specs = (P(("groups", "blk"), None), P(("groups", "blk")))
    return jax.shard_map(local, mesh=mesh, in_specs=in_specs, out_specs=out_specs, check_vma=False)
```
